256 devices in a mesh: scan: 8 (over y, core), ascan: 32 (over x, z).
Axes of the slice: x: 4, y: 4, z: 8, core: 2. Of those that a mesh axis runs over, the one named last changes fastest.
Arguments:
- spectra: bfloat16 [16, 4, 4096, 2048], P('scan', None, 'ascan'), may hold values from -8 to 8
- surface_top: int32 [16, 4096], P('scan', 'ascan'), may hold values from 0 to 3, as said below
- surface_bottom: int32 [16, 4096], P('scan', 'ascan'), may hold values from 1 to 8, as said below
Outputs:
- angiogram: float32 [16, 1024, 4096], P('scan', 'ascan')
- structure_map: float32 [16, 1024, 4096], P('scan', 'ascan')
- speckle_map: float32 [16, 1024, 4096], P('scan', 'ascan')
- mean_flow: float32 [], replicated
The draws below stay inside these ranges and needn't reach their ends.
Inputs may be any that keep to these rules, and one draw needn't show every extreme that they name: surface_top counts tiles of 128 depth rows. surface_bottom is greater than surface_top of the same A-scan.
All inputs are finite; a program needn't handle non-finite values.
Results may differ from the reference program's by a relative error of at most 0.0032.
Values sent between devices are 32-bit elements; how exact they have to be, the bound alone decides.
A program may use at most 128 MiB of HBM per device.

```python
import math
import jax
import jax.numpy as jnp
from jax import lax

REPEATS = 4
BINS = 2048
BANDS = 4
TILE = 128
BAND_BINS = 512
DEPTH = 1024
TILES = 8
NBSCAN = 16
ASCANS = 4096


def surfaces(key):
    first_key = jax.random.fold_in(key, 101)
    second_key = jax.random.fold_in(key, 202)
    surface_top = jax.random.randint(first_key, (NBSCAN, ASCANS), 0, TILES // 2, dtype=jnp.int32)
    position = jnp.arange(ASCANS, dtype=jnp.int32)[None, :]
    room_left = TILES - surface_top
    reach = 1 + (room_left - 1) * (position + 1) // ASCANS
    thickness = jax.random.randint(second_key, (NBSCAN, ASCANS), 1, reach + 1, dtype=jnp.int32)
    return (surface_top, surface_top + thickness)


def draw_surface_top(key, part):
    return surfaces(key)[0]


def draw_surface_bottom(key, part):
    return surfaces(key)[1]


def draw_spectra(key, part):
    phase_key = jax.random.fold_in(key, 303)
    stripe_key = jax.random.fold_in(key, 404)
    common_key = jax.random.fold_in(key, 505)
    own_key = jax.random.fold_in(key, 606)
    phase_shift = jax.random.uniform(phase_key, (NBSCAN, 1), jnp.float32)
    position = jnp.arange(ASCANS, dtype=jnp.float32)[None, :] / ASCANS
    wave = jnp.sin(2.0 * math.pi * (position + phase_shift))
    correlation = 0.5 + 0.45 * wave
    vessel = jax.random.bernoulli(stripe_key, 0.15, (NBSCAN, ASCANS))
    correlation = jnp.where(vessel, 0.0, correlation)
    shared_part = jnp.sqrt(correlation)[:, None, :, None]
    own_part = jnp.sqrt(1.0 - correlation)[:, None, :, None]
    common = jax.random.normal(common_key, (NBSCAN, 1, ASCANS, BINS), jnp.float32)
    own = jax.random.normal(own_key, (NBSCAN, REPEATS, ASCANS, BINS), jnp.float32)
    mixed = jnp.clip(shared_part * common + own_part * own, -6.0, 6.0)
    return mixed.astype(jnp.bfloat16)


def setup_inputs(seed: int = 0) -> dict:
    keys = jax.random.split(jax.random.key(seed), 4)
    return {
        "spectra": draw_spectra(jax.random.fold_in(keys[3], 71), 0),
        "surface_top": draw_surface_top(jax.random.fold_in(keys[3], 71), 0),
        "surface_bottom": draw_surface_bottom(jax.random.fold_in(keys[3], 71), 0),
    }


FLOOR_SHARE = 0.05
VARIANCE_SCALE = 0.1

def make_table():
    sample = jnp.arange(BAND_BINS, dtype=jnp.int32)
    depth_index = jnp.arange(DEPTH, dtype=jnp.int32)
    product = sample[:, None] * depth_index[None, :] % BINS
    phase_angle = product.astype(jnp.float32) * (2.0 * math.pi / BINS)
    window = jnp.sin(math.pi * (sample.astype(jnp.float32) + 0.5) / BAND_BINS) ** 2
    cosine = window[:, None] * jnp.cos(phase_angle)
    sine = window[:, None] * jnp.sin(phase_angle)
    return jnp.concatenate([cosine, sine], axis=1).astype(jnp.bfloat16)

def band_moments(spectra, table_part, first_row, surface_top, surface_bottom):
    scan_count, repeat_count, ascan_count, bin_count = spectra.shape
    depth_width = table_part.shape[1] // 2
    flat = spectra.reshape(scan_count * repeat_count * ascan_count, BANDS, BAND_BINS)
    similarity_total = jnp.zeros((scan_count, ascan_count, depth_width), jnp.float32)
    amplitude_total = jnp.zeros((scan_count, ascan_count, depth_width), jnp.float32)
    variance_total = jnp.zeros((scan_count, ascan_count, depth_width), jnp.float32)
    for band_index in range(BANDS):
        profile = jnp.dot(flat[:, band_index, :], table_part, preferred_element_type=jnp.float32)
        profile = profile.reshape(scan_count, repeat_count, ascan_count, 2 * depth_width)
        amplitude = jnp.sqrt(profile[..., :depth_width] ** 2 + profile[..., depth_width:] ** 2)
        earlier = amplitude[:, :-1]
        later = amplitude[:, 1:]
        similarity = 2.0 * earlier * later / jnp.maximum(earlier ** 2 + later ** 2, FLOOR_SHARE * BAND_BINS)
        similarity_total = similarity_total + lax.optimization_barrier(jnp.sum(similarity, axis=1))
        amplitude_total = amplitude_total + lax.optimization_barrier(jnp.sum(amplitude, axis=1))
        repeat_mean = lax.optimization_barrier(jnp.mean(amplitude, axis=1, keepdims=True))
        variance_total = variance_total + lax.optimization_barrier(jnp.mean((amplitude - repeat_mean) ** 2, axis=1))
    depth_rows = first_row + jnp.arange(depth_width, dtype=jnp.int32)
    lower = depth_rows[None, None, :] >= surface_top[..., None] * TILE
    upper = depth_rows[None, None, :] < surface_bottom[..., None] * TILE
    inside = (lower & upper).astype(jnp.float32)
    decorrelation = (1.0 - similarity_total / (BANDS * (REPEATS - 1))) * inside
    structure = amplitude_total / (BANDS * REPEATS) / math.sqrt(BAND_BINS) * inside
    speckle = variance_total / BANDS / (VARIANCE_SCALE * BAND_BINS) * inside
    return (decorrelation, structure, speckle, jnp.sum(decorrelation), jnp.sum(inside))

def reference(spectra, surface_top, surface_bottom):
    dft_table = make_table()

    def one_scan(items):
        scan_spectra, scan_top, scan_bottom = items
        return band_moments(scan_spectra[None], dft_table, 0, scan_top[None], scan_bottom[None])
    decorrelation, structure, speckle, flow_sums, tissue_counts = lax.map(one_scan, (spectra, surface_top, surface_bottom))
    decorrelation = decorrelation[:, 0]
    structure = structure[:, 0]
    speckle = speckle[:, 0]
    mean_flow = jnp.sum(flow_sums) / jnp.sum(tissue_counts)
    padded = jnp.pad(decorrelation, ((0, 0), (1, 1), (0, 0)))
    smoothed = (padded[:, :-2] + padded[:, 1:-1] + padded[:, 2:]) / 3.0
    angiogram = jnp.swapaxes(smoothed / mean_flow, 1, 2)
    return (angiogram, jnp.swapaxes(structure, 1, 2), jnp.swapaxes(speckle, 1, 2), mean_flow)
```

```python
import functools
import math

import jax
import jax.numpy as jnp
import numpy as np
from jax import lax
from jax.experimental import pallas as pl
from jax.experimental.pallas import tpu as pltpu
from jax.sharding import PartitionSpec as P

REPEATS = 4
BINS = 2048
BANDS = 4
TILE = 128
BAND_BINS = 512
DEPTH = 1024
TILES = DEPTH // TILE
FLOOR = 0.05 * BAND_BINS
VARIANCE_SCALE = 0.1
TINY = float(np.finfo(np.float32).tiny)

MESH = pl.DeviceIdType.MESH
CHUNK = 32


def make_table():
    sample = np.arange(BAND_BINS, dtype=np.int32)
    depth = np.arange(DEPTH, dtype=np.int32)
    product = sample[:, None] * depth[None, :] % BINS
    angle = product.astype(np.float32) * np.float32(2.0 * math.pi / BINS)
    window = np.sin(np.float32(math.pi) * (sample.astype(np.float32) + np.float32(0.5)) / np.float32(BAND_BINS)) ** 2
    parts = np.stack([window[:, None] * np.cos(angle), window[:, None] * np.sin(angle)])
    parts = parts.reshape(2, BAND_BINS, TILES, TILE).transpose(2, 1, 0, 3)
    return jnp.asarray(parts.reshape(TILES, BAND_BINS, 2 * TILE), dtype=jnp.bfloat16)


def exchange_kernel(
    n_scan, n_ascan, scans, slab,
    spectra_ref, table_ref, top_ref, bottom_ref,
    maps_ref, stat_ref,
    profile, moments, outbox, flow, own_stat, line_stat, stat_a, stat_b,
    send_sem, recv_sem, own_sem, send_a, recv_a, send_b, recv_b,
):
    my_scan = lax.axis_index("scan")
    me = lax.axis_index("ascan")
    per_tile = TILE // slab

    barrier = pltpu.get_barrier_semaphore()

    @pl.loop(1, n_ascan)
    def _(d):
        pl.semaphore_signal(barrier, inc=1, device_id=(my_scan, lax.rem(me + d, n_ascan)), device_id_type=MESH)

    @pl.loop(1, n_scan)
    def _(d):
        pl.semaphore_signal(barrier, inc=1, device_id=(lax.rem(my_scan + d, n_scan), me), device_id_type=MESH)

    pl.semaphore_wait(barrier, n_ascan + n_scan - 2)

    flow[...] = jnp.zeros_like(flow)
    first_tile = me // per_tile

    def block_copy(tile, q, s, source, to):
        return pltpu.make_async_remote_copy(
            src_ref=outbox.at[tile, q, s],
            dst_ref=maps_ref.at[:, s, :, pl.ds(pl.multiple_of(source * TILE, TILE), TILE)],
            send_sem=send_sem.at[tile * per_tile + q, s],
            recv_sem=recv_sem.at[source, s],
            device_id=(my_scan, to),
            device_id_type=MESH,
        )

    def own_copy(s):
        return pltpu.make_async_copy(
            outbox.at[me // per_tile, lax.rem(me, per_tile), s],
            maps_ref.at[:, s, :, pl.ds(pl.multiple_of(me * TILE, TILE), TILE)],
            own_sem.at[s],
        )

    @pl.loop(0, TILES * scans)
    def _(step):
        tile = lax.rem(first_tile + 1 + step // scans, TILES)
        s = lax.rem(step, scans)
        table = table_ref[tile]
        for band in range(BANDS):
            rows = spectra_ref[s, :, :, band * BAND_BINS : (band + 1) * BAND_BINS]
            profile[band] = jnp.dot(
                rows.reshape(REPEATS * TILE, BAND_BINS), table, preferred_element_type=jnp.float32
            )

        @pl.loop(0, TILE // CHUNK)
        def _(chunk):
            similarity = jnp.zeros((CHUNK, TILE), jnp.float32)
            total = jnp.zeros((CHUNK, TILE), jnp.float32)
            near = jnp.zeros((CHUNK, TILE), jnp.float32)
            far = jnp.zeros((CHUNK, TILE), jnp.float32)
            for band in range(BANDS):
                power, amplitude = [], []
                for r in range(REPEATS):
                    at = pl.ds(pl.multiple_of(r * TILE + chunk * CHUNK, CHUNK), CHUNK)
                    c = profile[band, at, :TILE]
                    v = profile[band, at, TILE:]
                    p = c * c + v * v
                    power.append(p)
                    amplitude.append(p * lax.rsqrt(jnp.maximum(p, TINY)))
                for r in range(REPEATS - 1):
                    root = lax.rsqrt(jnp.maximum(power[r] + power[r + 1], FLOOR))
                    similarity += (amplitude[r] * root) * (amplitude[r + 1] * root)
                first = amplitude[0] + amplitude[1]
                second = amplitude[2] + amplitude[3]
                total += first + second
                d0 = amplitude[0] - amplitude[1]
                d1 = amplitude[2] - amplitude[3]
                d2 = first - second
                near += d0 * d0 + d1 * d1
                far += d2 * d2
            at = pl.ds(pl.multiple_of(chunk * CHUNK, CHUNK), CHUNK)
            moments[0, at, :] = 1.0 - similarity * (2.0 / (BANDS * (REPEATS - 1)))
            moments[1, at, :] = total * (1.0 / (BANDS * REPEATS * math.sqrt(BAND_BINS)))
            moments[2, at, :] = (near * 0.5 + far * 0.25) * (
                1.0 / (REPEATS * BANDS * VARIANCE_SCALE * BAND_BINS)
            )

        top = top_ref[pl.ds(s, 1), :]
        bottom = bottom_ref[pl.ds(s, 1), :]
        inside = ((top <= tile) & (tile < bottom)).astype(jnp.float32)
        for m in range(3):
            turned = moments[m].T * inside
            if m == 0:
                flow[...] += jnp.sum(turned.reshape(TILE // 8, 8, TILE), axis=0)
            for q in range(per_tile):
                outbox[tile, q, s, m] = turned[q * slab : (q + 1) * slab]

        @pl.loop(0, per_tile)
        def _(q):
            to = tile * per_tile + q

            @pl.when(to != me)
            def _():
                block_copy(tile, q, s, me, to).start()

            @pl.when(to == me)
            def _():
                own_copy(s).start()

    own_stat[pl.ds(0, 8), :] = flow[...]
    rows = (bottom_ref[...] - top_ref[...]).astype(jnp.float32) * float(TILE)
    own_stat[pl.ds(8, 8), :] = jnp.concatenate([rows, jnp.zeros((8 - scans, TILE), jnp.float32)], axis=0)
    stat_a[my_scan] = own_stat[...]

    def a_copy(source, to, k):
        return pltpu.make_async_remote_copy(
            src_ref=own_stat, dst_ref=stat_a.at[source],
            send_sem=send_a.at[k], recv_sem=recv_a.at[source],
            device_id=(to, me), device_id_type=MESH,
        )

    def b_copy(source, to, k):
        return pltpu.make_async_remote_copy(
            src_ref=line_stat, dst_ref=stat_b.at[source],
            send_sem=send_b.at[k], recv_sem=recv_b.at[source],
            device_id=(my_scan, to), device_id_type=MESH,
        )

    @pl.loop(1, n_scan)
    def _(d):
        a_copy(my_scan, lax.rem(my_scan + d, n_scan), d).start()

    @pl.loop(1, n_scan)
    def _(d):
        a_copy(lax.rem(my_scan + d, n_scan), lax.rem(my_scan + d, n_scan), d).wait_recv()

    line_stat[...] = jnp.sum(stat_a[...], axis=0)
    stat_b[me] = line_stat[...]

    @pl.loop(1, n_ascan)
    def _(d):
        b_copy(me, lax.rem(me + d, n_ascan), d).start()

    @pl.loop(1, n_scan)
    def _(d):
        a_copy(my_scan, lax.rem(my_scan + d, n_scan), d).wait_send()

    for s in range(scans):
        own_copy(s).wait()

    @pl.loop(1, n_ascan)
    def _(d):
        other = lax.rem(me + d, n_ascan)
        b_copy(other, other, d).wait_recv()
        for s in range(scans):
            block_copy(other // per_tile, lax.rem(other, per_tile), s, other, other).wait_recv()

    stat_ref[...] = jnp.sum(stat_b[...], axis=0)

    @pl.loop(1, n_ascan)
    def _(d):
        other = lax.rem(me + d, n_ascan)
        b_copy(me, other, d).wait_send()
        for s in range(scans):
            block_copy(other // per_tile, lax.rem(other, per_tile), s, me, other).wait_send()


def finish_kernel(maps_ref, stat_ref, angiogram_ref, structure_ref, speckle_ref, mean_ref):
    flow = jnp.sum(stat_ref[pl.ds(0, 8), :], keepdims=True)
    count = jnp.sum(stat_ref[pl.ds(8, 8), :], keepdims=True)
    mean = flow / count
    x = maps_ref[0, 0]
    width = x.shape[1]
    lane = lax.broadcasted_iota(jnp.int32, x.shape, 1)
    before = jnp.where(lane == 0, 0.0, pltpu.roll(x, 1, 1))
    after = jnp.where(lane == width - 1, 0.0, pltpu.roll(x, width - 1, 1))
    angiogram_ref[0] = (before + x + after) * (1.0 / (3.0 * mean))
    structure_ref[0] = maps_ref[1, 0]
    speckle_ref[0] = maps_ref[2, 0]
    mean_ref[...] = mean


def solution(mesh):
    n_scan, n_ascan = mesh.shape["scan"], mesh.shape["ascan"]

    def body(spectra, top, bottom):
        scans, repeats, lines, bins = spectra.shape
        slab = DEPTH // n_ascan
        width = lines * n_ascan
        f32 = jnp.float32
        vmem = pl.BlockSpec(memory_space=pltpu.VMEM)
        maps, stat = pl.pallas_call(
            functools.partial(exchange_kernel, n_scan, n_ascan, scans, slab),
            out_shape=(
                jax.ShapeDtypeStruct((3, scans, slab, width), f32),
                jax.ShapeDtypeStruct((16, TILE), f32),
            ),
            in_specs=[vmem] * 4,
            out_specs=(pl.BlockSpec(memory_space=pl.ANY), vmem),
            scratch_shapes=[
                pltpu.VMEM((BANDS, REPEATS * TILE, 2 * TILE), f32),
                pltpu.VMEM((3, TILE, TILE), f32),
                pltpu.VMEM((TILES, TILE // slab, scans, 3, slab, TILE), f32),
                pltpu.VMEM((8, TILE), f32),
                pltpu.VMEM((16, TILE), f32),
                pltpu.VMEM((16, TILE), f32),
                pltpu.VMEM((n_scan, 16, TILE), f32),
                pltpu.VMEM((n_ascan, 16, TILE), f32),
                pltpu.SemaphoreType.DMA((n_ascan, scans)),
                pltpu.SemaphoreType.DMA((n_ascan, scans)),
                pltpu.SemaphoreType.DMA((scans,)),
                pltpu.SemaphoreType.DMA((n_scan,)),
                pltpu.SemaphoreType.DMA((n_scan,)),
                pltpu.SemaphoreType.DMA((n_ascan,)),
                pltpu.SemaphoreType.DMA((n_ascan,)),
            ],
            compiler_params=pltpu.CompilerParams(
                collective_id=0, has_side_effects=True, vmem_limit_bytes=32 * 2**20
            ),
            name="exchange",
        )(spectra, make_table(), top, bottom)

        block = 16
        out_spec = pl.BlockSpec((1, block, width), lambda s, k: (s, k, 0))
        angiogram, structure, speckle, mean = pl.pallas_call(
            finish_kernel,
            grid=(scans, slab // block),
            out_shape=[jax.ShapeDtypeStruct((scans, slab, width), f32)] * 3
            + [jax.ShapeDtypeStruct((1, 1), f32)],
            in_specs=[
                pl.BlockSpec((3, 1, block, width), lambda s, k: (0, s, k, 0)),
                pl.BlockSpec((16, TILE), lambda s, k: (0, 0)),
            ],
            out_specs=[out_spec] * 3 + [pl.BlockSpec((1, 1), lambda s, k: (0, 0))],
            name="finish",
        )(maps, stat)
        return angiogram, structure, speckle, mean.reshape(())

    return jax.shard_map(
        body,
        mesh=mesh,
        in_specs=(P("scan", None, "ascan", None), P("scan", "ascan"), P("scan", "ascan")),
        out_specs=(P("scan", "ascan", None),) * 3 + (P(),),
        check_vma=False,
    )
```

```python
import functools
import math

import jax
import jax.numpy as jnp
import numpy as np
from jax import lax
from jax.experimental import pallas as pl
from jax.experimental.pallas import tpu as pltpu
from jax.sharding import PartitionSpec as P

REPEATS = 4
BINS = 2048
BANDS = 4
TILE = 128
BAND_BINS = 512
DEPTH = 1024
TILES = DEPTH // TILE
FLOOR = 0.05 * BAND_BINS
VARIANCE_SCALE = 0.1
TINY = float(np.finfo(np.float32).tiny)

MESH = pl.DeviceIdType.MESH
CHUNK = 32


def make_table():
    sample = np.arange(BAND_BINS, dtype=np.int32)
    depth = np.arange(DEPTH, dtype=np.int32)
    product = sample[:, None] * depth[None, :] % BINS
    angle = product.astype(np.float32) * np.float32(2.0 * math.pi / BINS)
    window = np.sin(np.float32(math.pi) * (sample.astype(np.float32) + np.float32(0.5)) / np.float32(BAND_BINS)) ** 2
    parts = np.stack([window[:, None] * np.cos(angle), window[:, None] * np.sin(angle)])
    parts = parts.reshape(2, BAND_BINS, TILES, TILE).transpose(2, 1, 0, 3)
    return jnp.asarray(parts.reshape(TILES, BAND_BINS, 2 * TILE), dtype=jnp.bfloat16)


def exchange_kernel(
    n_scan, n_ascan, scans, slab,
    spectra_hbm, table_hbm, top_hbm, bottom_hbm,
    maps_ref, stat_ref,
    spectra, table, top_ref, bottom_ref, profile, sums, outbox, flow, own_stat, line_stat, stat_a, stat_b,
    spectra_sem, table_sem, surface_sem, send_sem, recv_sem, own_sem, send_a, recv_a, send_b, recv_b,
):
    my_scan = lax.axis_index("scan")
    me = lax.axis_index("ascan")
    per_tile = TILE // slab
    first_tile = lax.rem(me // per_tile + 1, TILES)

    barrier = pltpu.get_barrier_semaphore()

    @pl.loop(1, n_ascan)
    def _(d):
        pl.semaphore_signal(barrier, inc=1, device_id=(my_scan, lax.rem(me + d, n_ascan)), device_id_type=MESH)

    @pl.loop(1, n_scan)
    def _(d):
        pl.semaphore_signal(barrier, inc=1, device_id=(lax.rem(my_scan + d, n_scan), me), device_id_type=MESH)

    def table_copy(tile):
        return pltpu.make_async_copy(table_hbm.at[tile], table.at[tile], table_sem.at[tile])

    def spectra_copy(s, band):
        bins = pl.ds(band * BAND_BINS, BAND_BINS)
        return pltpu.make_async_copy(
            spectra_hbm.at[s, :, :, bins], spectra.at[s, band], spectra_sem.at[s, band]
        )

    surface_copies = (
        pltpu.make_async_copy(top_hbm, top_ref, surface_sem.at[0]),
        pltpu.make_async_copy(bottom_hbm, bottom_ref, surface_sem.at[1]),
    )
    table_copy(first_tile).start()
    for s in range(scans):
        for band in range(BANDS):
            spectra_copy(s, band).start()
        if s == 0:
            for c in surface_copies:
                c.start()

    @pl.loop(1, TILES)
    def _(d):
        table_copy(lax.rem(first_tile + d, TILES)).start()

    flow[...] = jnp.zeros_like(flow)

    def block_copy(tile, q, s, source, to):
        return pltpu.make_async_remote_copy(
            src_ref=outbox.at[tile, q, s],
            dst_ref=maps_ref.at[:, s, :, pl.ds(pl.multiple_of(source * TILE, TILE), TILE)],
            send_sem=send_sem.at[tile * per_tile + q, s],
            recv_sem=recv_sem.at[source, s],
            device_id=(my_scan, to),
            device_id_type=MESH,
        )

    def own_copy(s):
        return pltpu.make_async_copy(
            outbox.at[me // per_tile, lax.rem(me, per_tile), s],
            maps_ref.at[:, s, :, pl.ds(pl.multiple_of(me * TILE, TILE), TILE)],
            own_sem.at[s],
        )

    def band_terms(band, at):
        power, amplitude = [], []
        for r in range(REPEATS):
            rows = pl.ds(r * TILE + at, CHUNK)
            c = profile[band, rows, :TILE]
            v = profile[band, rows, TILE:]
            p = c * c + v * v
            power.append(p)
            amplitude.append(p * lax.rsqrt(jnp.maximum(p, TINY)))
        similarity = None
        for r in range(REPEATS - 1):
            root = lax.rsqrt(jnp.maximum(power[r] + power[r + 1], FLOOR))
            term = (amplitude[r] * root) * (amplitude[r + 1] * root)
            similarity = term if similarity is None else similarity + term
        first = amplitude[0] + amplitude[1]
        second = amplitude[2] + amplitude[3]
        d0 = amplitude[0] - amplitude[1]
        d1 = amplitude[2] - amplitude[3]
        d2 = first - second
        return similarity, first + second, (d0 * d0 + d1 * d1) + (d2 * d2) * 0.5

    @pl.loop(0, TILES * scans)
    def _(step):
        tile = lax.rem(first_tile + step // scans, TILES)
        s = lax.rem(step, scans)

        @pl.when(s == 0)
        def _():
            table_copy(tile).wait()

        @pl.when(step < scans)
        def _():
            for band in range(BANDS):
                spectra_copy(s, band).wait()

        weights = table[tile]
        for band in range(BANDS):
            profile[band] = jnp.dot(
                spectra[s, band].reshape(REPEATS * TILE, BAND_BINS),
                weights,
                preferred_element_type=jnp.float32,
            )
            for at in range(0, TILE, CHUNK):
                terms = band_terms(band, at)
                for m in range(3):
                    rows = pl.ds(at, CHUNK)
                    sums[m, rows, :] = terms[m] if band == 0 else sums[m, rows, :] + terms[m]

        @pl.when(step == 0)
        def _():
            for c in surface_copies:
                c.wait()

        top = top_ref[pl.ds(s, 1), :]
        bottom = bottom_ref[pl.ds(s, 1), :]
        inside = ((top <= tile) & (tile < bottom)).astype(jnp.float32)
        for m in range(3):
            turned = sums[m].T
            if m == 0:
                turned = (1.0 - turned * (2.0 / (BANDS * (REPEATS - 1)))) * inside
                flow[...] += jnp.sum(turned.reshape(TILE // 8, 8, TILE), axis=0)
            elif m == 1:
                turned = turned * (inside * (1.0 / (BANDS * REPEATS * math.sqrt(BAND_BINS))))
            else:
                turned = turned * (inside * (0.5 / (REPEATS * BANDS * VARIANCE_SCALE * BAND_BINS)))
            for q in range(per_tile):
                outbox[tile, q, s, m] = turned[q * slab : (q + 1) * slab]

        @pl.when(step == 0)
        def _():
            pl.semaphore_wait(barrier, n_ascan + n_scan - 2)

        @pl.loop(0, per_tile)
        def _(q):
            to = tile * per_tile + q

            @pl.when(to != me)
            def _():
                block_copy(tile, q, s, me, to).start()

            @pl.when(to == me)
            def _():
                own_copy(s).start()

    rows = jnp.sum((bottom_ref[...] - top_ref[...]).astype(jnp.float32), axis=0, keepdims=True)
    own_stat[pl.ds(0, 1), :] = jnp.sum(flow[...], axis=0, keepdims=True)
    own_stat[pl.ds(1, 1), :] = rows * float(TILE)
    stat_a[my_scan] = own_stat[...]

    def a_copy(source, to, k):
        return pltpu.make_async_remote_copy(
            src_ref=own_stat, dst_ref=stat_a.at[source],
            send_sem=send_a.at[k], recv_sem=recv_a.at[source],
            device_id=(to, me), device_id_type=MESH,
        )

    def b_copy(source, to, k):
        return pltpu.make_async_remote_copy(
            src_ref=line_stat, dst_ref=stat_b.at[source],
            send_sem=send_b.at[k], recv_sem=recv_b.at[source],
            device_id=(my_scan, to), device_id_type=MESH,
        )

    @pl.loop(1, n_scan)
    def _(d):
        a_copy(my_scan, lax.rem(my_scan + d, n_scan), d).start()

    @pl.loop(1, n_scan)
    def _(d):
        a_copy(lax.rem(my_scan + d, n_scan), lax.rem(my_scan + d, n_scan), d).wait_recv()

    line_stat[...] = jnp.sum(stat_a[...], axis=0)
    stat_b[me] = line_stat[...]

    @pl.loop(1, n_ascan)
    def _(d):
        b_copy(me, lax.rem(me + d, n_ascan), d).start()

    @pl.loop(1, n_scan)
    def _(d):
        a_copy(my_scan, lax.rem(my_scan + d, n_scan), d).wait_send()

    @pl.loop(1, n_ascan)
    def _(d):
        other = lax.rem(me + d, n_ascan)
        b_copy(other, other, d).wait_recv()

    stat_ref[...] = jnp.sum(stat_b[...], axis=0)
    for s in range(scans):
        own_copy(s).wait()

    @pl.loop(1, n_ascan)
    def _(d):
        other = lax.rem(me + d, n_ascan)
        b_copy(me, other, d).wait_send()
        for s in range(scans):
            block_copy(other // per_tile, lax.rem(other, per_tile), s, me, other).wait_send()

    @pl.loop(1, n_ascan)
    def _(d):
        other = lax.rem(me + d, n_ascan)
        for s in range(scans):
            block_copy(other // per_tile, lax.rem(other, per_tile), s, other, other).wait_recv()


def finish_kernel(maps_ref, stat_ref, angiogram_ref, structure_ref, speckle_ref, mean_ref, maps, smooth, sem_in, sem_out):
    scans, slab, width = angiogram_ref.shape
    outs = (angiogram_ref, structure_ref, speckle_ref)
    reads = [[pltpu.make_async_copy(maps_ref.at[m, s], maps.at[m, s], sem_in.at[m, s]) for s in range(scans)] for m in range(3)]
    writes = [
        [
            pltpu.make_async_copy(smooth.at[s] if m == 0 else maps.at[m, s], outs[m].at[s], sem_out.at[m, s])
            for s in range(scans)
        ]
        for m in range(3)
    ]
    for m in range(3):
        for s in range(scans):
            reads[m][s].start()
    totals = jnp.sum(stat_ref[...], axis=1, keepdims=True)
    mean = totals[0:1] / totals[1:2]
    scale = 1.0 / (3.0 * mean)
    mean_ref[...] = mean
    lane = lax.broadcasted_iota(jnp.int32, (8, width), 1)
    for s in range(scans):
        reads[0][s].wait()
        for z in range(0, slab, 8):
            x = maps[0, s, pl.ds(z, 8), :]
            before = jnp.where(lane == 0, 0.0, pltpu.roll(x, 1, 1))
            after = jnp.where(lane == width - 1, 0.0, pltpu.roll(x, width - 1, 1))
            smooth[s, pl.ds(z, 8), :] = (before + x + after) * scale
        writes[0][s].start()
        for m in (1, 2):
            reads[m][s].wait()
            writes[m][s].start()
    for m in range(3):
        for s in range(scans):
            writes[m][s].wait()


def solution(mesh):
    n_scan, n_ascan = mesh.shape["scan"], mesh.shape["ascan"]

    def body(spectra, top, bottom):
        scans, repeats, lines, bins = spectra.shape
        slab = DEPTH // n_ascan
        width = lines * n_ascan
        f32 = jnp.float32
        vmem = pl.BlockSpec(memory_space=pltpu.VMEM)
        hbm = pl.BlockSpec(memory_space=pltpu.HBM)
        maps, stat = pl.pallas_call(
            functools.partial(exchange_kernel, n_scan, n_ascan, scans, slab),
            out_shape=(
                jax.ShapeDtypeStruct((3, scans, slab, width), f32),
                jax.ShapeDtypeStruct((2, TILE), f32),
            ),
            in_specs=[hbm] * 4,
            out_specs=(hbm, vmem),
            scratch_shapes=[
                pltpu.VMEM((scans, BANDS, REPEATS, TILE, BAND_BINS), jnp.bfloat16),
                pltpu.VMEM((TILES, BAND_BINS, 2 * TILE), jnp.bfloat16),
                pltpu.VMEM((scans, TILE), jnp.int32),
                pltpu.VMEM((scans, TILE), jnp.int32),
                pltpu.VMEM((BANDS, REPEATS * TILE, 2 * TILE), f32),
                pltpu.VMEM((3, TILE, TILE), f32),
                pltpu.VMEM((TILES, TILE // slab, scans, 3, slab, TILE), f32),
                pltpu.VMEM((8, TILE), f32),
                pltpu.VMEM((2, TILE), f32),
                pltpu.VMEM((2, TILE), f32),
                pltpu.VMEM((n_scan, 2, TILE), f32),
                pltpu.VMEM((n_ascan, 2, TILE), f32),
                pltpu.SemaphoreType.DMA((scans, BANDS)),
                pltpu.SemaphoreType.DMA((TILES,)),
                pltpu.SemaphoreType.DMA((2,)),
                pltpu.SemaphoreType.DMA((n_ascan, scans)),
                pltpu.SemaphoreType.DMA((n_ascan, scans)),
                pltpu.SemaphoreType.DMA((scans,)),
                pltpu.SemaphoreType.DMA((n_scan,)),
                pltpu.SemaphoreType.DMA((n_scan,)),
                pltpu.SemaphoreType.DMA((n_ascan,)),
                pltpu.SemaphoreType.DMA((n_ascan,)),
            ],
            compiler_params=pltpu.CompilerParams(
                collective_id=0, has_side_effects=True, vmem_limit_bytes=58 * 2**20
            ),
            name="exchange",
        )(spectra, make_table(), top, bottom)

        angiogram, structure, speckle, mean = pl.pallas_call(
            finish_kernel,
            out_shape=[jax.ShapeDtypeStruct((scans, slab, width), f32)] * 3
            + [jax.ShapeDtypeStruct((1, 1), f32)],
            in_specs=[hbm, vmem],
            out_specs=[hbm] * 3 + [vmem],
            scratch_shapes=[
                pltpu.VMEM((3, scans, slab, width), f32),
                pltpu.VMEM((scans, slab, width), f32),
                pltpu.SemaphoreType.DMA((3, scans)),
                pltpu.SemaphoreType.DMA((3, scans)),
            ],
            name="finish",
        )(maps, stat)
        return angiogram, structure, speckle, mean.reshape(())

    return jax.shard_map(
        body,
        mesh=mesh,
        in_specs=(P("scan", None, "ascan", None), P("scan", "ascan"), P("scan", "ascan")),
        out_specs=(P("scan", "ascan", None),) * 3 + (P(),),
        check_vma=False,
    )
```

```python
import functools
import math

import jax
import jax.numpy as jnp
import numpy as np
from jax import lax
from jax.experimental import pallas as pl
from jax.experimental.pallas import tpu as pltpu
from jax.sharding import PartitionSpec as P

REPEATS = 4
BINS = 2048
BANDS = 4
TILE = 128
BAND_BINS = 512
DEPTH = 1024
TILES = DEPTH // TILE
FLOOR = 0.05 * BAND_BINS
VARIANCE_SCALE = 0.1
TINY = float(np.finfo(np.float32).tiny)

MESH = pl.DeviceIdType.MESH
CHUNK = 32
SLAB = 32
RING = 8
HELD = 4


def make_table():
    sample = np.arange(BAND_BINS, dtype=np.int32)
    depth = np.arange(DEPTH, dtype=np.int32)
    product = sample[:, None] * depth[None, :] % BINS
    angle = product.astype(np.float32) * np.float32(2.0 * math.pi / BINS)
    window = np.sin(np.float32(math.pi) * (sample.astype(np.float32) + np.float32(0.5)) / np.float32(BAND_BINS)) ** 2
    parts = np.stack([window[:, None] * np.cos(angle), window[:, None] * np.sin(angle)])
    parts = parts.reshape(2, BAND_BINS, TILE // SLAB, RING, SLAB).transpose(3, 1, 0, 2, 4)
    return jnp.asarray(parts.reshape(RING, BAND_BINS, 2 * TILE), dtype=jnp.bfloat16)


def exchange_kernel(
    n_scan, n_ascan, scans, slab,
    spectra_hbm, table_hbm, top_hbm, bottom_hbm,
    maps_ref, stat_ref,
    spectra, table, top_ref, bottom_ref, profile, sums, outbox, flow, own_stat, line_stat, stat_a, stat_b,
    spectra_sem, table_sem, surface_sem, send_sem, recv_sem, send_a, recv_a, send_b, recv_b,
):
    my_scan = lax.axis_index("scan")
    me = lax.axis_index("ascan")
    per_tile = TILE // slab
    row, place = me // RING, lax.rem(me, RING)

    def group_of(step):
        pair = step // (2 * scans)
        reach = jnp.where(pair == 0, 2, jnp.where(pair == 1, 1, 3))
        near = jnp.where(lax.rem(step, 2) == 0, reach, RING - reach)
        distance = jnp.where(step < 6 * scans, near, jnp.where(step < 7 * scans, 4, 0))
        return lax.rem(place + distance, RING)

    def scan_of(step):
        return jnp.where(step < 6 * scans, lax.rem(step // 2, scans), lax.rem(step, scans))


    barrier = pltpu.get_barrier_semaphore()

    @pl.loop(1, n_ascan)
    def _(d):
        pl.semaphore_signal(barrier, inc=1, device_id=(my_scan, lax.rem(me + d, n_ascan)), device_id_type=MESH)

    @pl.loop(1, n_scan)
    def _(d):
        pl.semaphore_signal(barrier, inc=1, device_id=(lax.rem(my_scan + d, n_scan), me), device_id_type=MESH)

    def table_copy(tile):
        return pltpu.make_async_copy(table_hbm.at[tile], table.at[tile], table_sem.at[tile])

    def spectra_copy(s, band):
        bins = pl.ds(band * BAND_BINS, BAND_BINS)
        return pltpu.make_async_copy(
            spectra_hbm.at[s, :, :, bins], spectra.at[s, band], spectra_sem.at[s, band]
        )

    surface_copies = (
        pltpu.make_async_copy(top_hbm, top_ref, surface_sem.at[0]),
        pltpu.make_async_copy(bottom_hbm, bottom_ref, surface_sem.at[1]),
    )
    table_copy(group_of(0)).start()
    for s in range(scans):
        for band in range(BANDS):
            spectra_copy(s, band).start()
        if s == 0:
            for c in surface_copies:
                c.start()

    @pl.loop(1, RING)
    def _(d):
        table_copy(group_of(jnp.where(d < 6, d // 2 * (2 * scans) + lax.rem(d, 2), d * scans))).start()

    flow[...] = jnp.zeros_like(flow)

    def block_copy(s, source, to):
        return pltpu.make_async_remote_copy(
            src_ref=outbox.at[to, s],
            dst_ref=maps_ref.at[:, s, :, pl.ds(pl.multiple_of(source * TILE, TILE), TILE)],
            send_sem=send_sem.at[to, s],
            recv_sem=recv_sem.at[source, s],
            device_id=(my_scan, to),
            device_id_type=MESH,
        )

    def send(group, s):
        @pl.loop(0, per_tile)
        def _(d):
            to = lax.rem(row + d, per_tile) * RING + group

            @pl.when(to != me)
            def _():
                block_copy(s, me, to).start()

            @pl.when(to == me)
            def _():
                maps_ref[:, s, :, pl.ds(pl.multiple_of(me * TILE, TILE), TILE)] = outbox[me, s]

    def band_terms(band, at):
        power, amplitude = [], []
        for r in range(REPEATS):
            rows = pl.ds(r * TILE + at, CHUNK)
            c = profile[band, rows, :TILE]
            v = profile[band, rows, TILE:]
            p = c * c + v * v
            power.append(p)
            amplitude.append(p * lax.rsqrt(jnp.maximum(p, TINY)))
        similarity = None
        for r in range(REPEATS - 1):
            root = lax.rsqrt(jnp.maximum(power[r] + power[r + 1], FLOOR))
            term = (amplitude[r] * root) * (amplitude[r + 1] * root)
            similarity = term if similarity is None else similarity + term
        first = amplitude[0] + amplitude[1]
        second = amplitude[2] + amplitude[3]
        d0 = amplitude[0] - amplitude[1]
        d1 = amplitude[2] - amplitude[3]
        d2 = first - second
        return similarity, first + second, (d0 * d0 + d1 * d1) + (d2 * d2) * 0.5

    @pl.loop(0, RING * scans)
    def _(step):
        group, s = group_of(step), scan_of(step)

        @pl.when(s == 0)
        def _():
            table_copy(group).wait()

        @pl.when((step == 0) | (step == 2))
        def _():
            for band in range(BANDS):
                spectra_copy(s, band).wait()

        weights = table[group]
        for band in range(BANDS):

            profile[band] = jnp.dot(
                spectra[s, band].reshape(REPEATS * TILE, BAND_BINS),
                weights,
                preferred_element_type=jnp.float32,
            )
            for at in range(0, TILE, CHUNK):
                terms = band_terms(band, at)
                for m in range(3):
                    rows = pl.ds(at, CHUNK)
                    sums[m, rows, :] = terms[m] if band == 0 else sums[m, rows, :] + terms[m]

        @pl.when(step == 0)
        def _():
            for c in surface_copies:
                c.wait()

        top = top_ref[pl.ds(s, 1), :]
        bottom = bottom_ref[pl.ds(s, 1), :]
        masks = []
        for q in range(per_tile):
            tile = (q * RING + group) * slab // TILE
            masks.append(((top <= tile) & (tile < bottom)).astype(jnp.float32))
        for m in range(3):
            turned = sums[m].T
            for q in range(per_tile):
                part = turned[q * slab : (q + 1) * slab]
                if m == 0:
                    part = (1.0 - part * (2.0 / (BANDS * (REPEATS - 1)))) * masks[q]
                    flow[...] += jnp.sum(part.reshape(slab // 8, 8, TILE), axis=0)
                elif m == 1:
                    part = part * (masks[q] * (1.0 / (BANDS * REPEATS * math.sqrt(BAND_BINS))))
                else:
                    part = part * (masks[q] * (0.5 / (REPEATS * BANDS * VARIANCE_SCALE * BAND_BINS)))
                outbox[q * RING + group, s, m] = part

        @pl.when(step == 0)
        def _():
            pl.semaphore_wait(barrier, n_ascan + n_scan - 2)

        @pl.when(step < RING * scans - HELD)
        def _():
            send(group, s)

    rows = jnp.sum((bottom_ref[...] - top_ref[...]).astype(jnp.float32), axis=0, keepdims=True)
    own_stat[pl.ds(0, 1), :] = jnp.sum(flow[...], axis=0, keepdims=True)
    own_stat[pl.ds(1, 1), :] = rows * float(TILE)
    stat_a[my_scan] = own_stat[...]

    def a_copy(source, to, k):
        return pltpu.make_async_remote_copy(
            src_ref=own_stat, dst_ref=stat_a.at[source],
            send_sem=send_a.at[k], recv_sem=recv_a.at[source],
            device_id=(to, me), device_id_type=MESH,
        )

    def b_copy(source, to, k):
        return pltpu.make_async_remote_copy(
            src_ref=line_stat, dst_ref=stat_b.at[source],
            send_sem=send_b.at[k], recv_sem=recv_b.at[source],
            device_id=(my_scan, to), device_id_type=MESH,
        )

    @pl.loop(1, n_scan)
    def _(d):
        a_copy(my_scan, lax.rem(my_scan + d, n_scan), d).start()

    @pl.loop(1, n_scan)
    def _(d):
        a_copy(lax.rem(my_scan + d, n_scan), lax.rem(my_scan + d, n_scan), d).wait_recv()

    line_stat[...] = jnp.sum(stat_a[...], axis=0)
    stat_b[me] = line_stat[...]

    @pl.loop(1, n_ascan)
    def _(d):
        b_copy(me, lax.rem(me + d, n_ascan), d).start()

    @pl.loop(RING * scans - HELD, RING * scans)
    def _(step):
        send(group_of(step), scan_of(step))

    @pl.loop(1, n_scan)
    def _(d):
        a_copy(my_scan, lax.rem(my_scan + d, n_scan), d).wait_send()

    @pl.loop(1, n_ascan)
    def _(d):
        other = lax.rem(me + d, n_ascan)
        b_copy(other, other, d).wait_recv()

    stat_ref[...] = jnp.sum(stat_b[...], axis=0)

    @pl.loop(1, n_ascan)
    def _(d):
        other = lax.rem(me + d, n_ascan)
        b_copy(me, other, d).wait_send()
        for s in range(scans):
            block_copy(s, me, other).wait_send()

    @pl.loop(1, n_ascan)
    def _(d):
        other = lax.rem(me + d, n_ascan)
        for s in range(scans):
            block_copy(s, other, other).wait_recv()


def finish_kernel(maps_ref, stat_ref, angiogram_ref, structure_ref, speckle_ref, mean_ref, smooth, plain_sem, smooth_sem):
    scans, slab, width = angiogram_ref.shape
    block = smooth.shape[2]
    copies = [
        pltpu.make_async_copy(maps_ref.at[1], structure_ref, plain_sem.at[0]),
        pltpu.make_async_copy(maps_ref.at[2], speckle_ref, plain_sem.at[1]),
    ]
    for c in copies:
        c.start()
    totals = jnp.sum(stat_ref[...], axis=1, keepdims=True)
    mean = totals[0:1] / totals[1:2]
    scale = 1.0 / (3.0 * mean)
    mean_ref[...] = mean
    lane = lax.broadcasted_iota(jnp.int32, (8, width), 1)
    for s in range(scans):
        for k in range(slab // block):
            for z in range(0, block, 8):
                x = maps_ref[0, s, pl.ds(k * block + z, 8), :]
                before = jnp.where(lane == 0, 0.0, pltpu.roll(x, 1, 1))
                after = jnp.where(lane == width - 1, 0.0, pltpu.roll(x, width - 1, 1))
                smooth[s, k, pl.ds(z, 8), :] = (before + x + after) * scale
            c = pltpu.make_async_copy(
                smooth.at[s, k], angiogram_ref.at[s, pl.ds(k * block, block)], smooth_sem.at[s, k]
            )
            c.start()
            copies.append(c)
    for c in copies:
        c.wait()


def solution(mesh):
    n_scan, n_ascan = mesh.shape["scan"], mesh.shape["ascan"]

    def body(spectra, top, bottom):
        scans, repeats, lines, bins = spectra.shape
        slab = DEPTH // n_ascan
        width = lines * n_ascan
        f32 = jnp.float32
        vmem = pl.BlockSpec(memory_space=pltpu.VMEM)
        hbm = pl.BlockSpec(memory_space=pltpu.HBM)
        maps, stat = pl.pallas_call(
            functools.partial(exchange_kernel, n_scan, n_ascan, scans, slab),
            out_shape=(
                jax.ShapeDtypeStruct((3, scans, slab, width), f32),
                jax.ShapeDtypeStruct((2, TILE), f32),
            ),
            in_specs=[hbm] * 4,
            out_specs=(vmem, vmem),
            scratch_shapes=[
                pltpu.VMEM((scans, BANDS, REPEATS, TILE, BAND_BINS), jnp.bfloat16),
                pltpu.VMEM((RING, BAND_BINS, 2 * TILE), jnp.bfloat16),
                pltpu.VMEM((scans, TILE), jnp.int32),
                pltpu.VMEM((scans, TILE), jnp.int32),
                pltpu.VMEM((BANDS, REPEATS * TILE, 2 * TILE), f32),
                pltpu.VMEM((3, TILE, TILE), f32),
                pltpu.VMEM((n_ascan, scans, 3, slab, TILE), f32),
                pltpu.VMEM((8, TILE), f32),
                pltpu.VMEM((2, TILE), f32),
                pltpu.VMEM((2, TILE), f32),
                pltpu.VMEM((n_scan, 2, TILE), f32),
                pltpu.VMEM((n_ascan, 2, TILE), f32),
                pltpu.SemaphoreType.DMA((scans, BANDS)),
                pltpu.SemaphoreType.DMA((RING,)),
                pltpu.SemaphoreType.DMA((2,)),
                pltpu.SemaphoreType.DMA((n_ascan, scans)),
                pltpu.SemaphoreType.DMA((n_ascan, scans)),
                pltpu.SemaphoreType.DMA((n_scan,)),
                pltpu.SemaphoreType.DMA((n_scan,)),
                pltpu.SemaphoreType.DMA((n_ascan,)),
                pltpu.SemaphoreType.DMA((n_ascan,)),
            ],
            compiler_params=pltpu.CompilerParams(
                collective_id=0, has_side_effects=True, vmem_limit_bytes=40 * 2**20
            ),
            name="exchange",
        )(*(pltpu.with_memory_space_constraint(a, pltpu.HBM) for a in (spectra, make_table(), top, bottom)))

        angiogram, structure, speckle, mean = pl.pallas_call(
            finish_kernel,
            out_shape=[jax.ShapeDtypeStruct((scans, slab, width), f32)] * 3
            + [jax.ShapeDtypeStruct((1, 1), f32)],
            in_specs=[vmem, vmem],
            out_specs=[hbm] * 3 + [vmem],
            scratch_shapes=[
                pltpu.VMEM((scans, slab // 16, 16, width), f32),
                pltpu.SemaphoreType.DMA((2,)),
                pltpu.SemaphoreType.DMA((scans, slab // 16)),
            ],
            compiler_params=pltpu.CompilerParams(vmem_limit_bytes=8 * 2**20),
            name="finish",
        )(maps, stat)
        return angiogram, structure, speckle, mean.reshape(())

    return jax.shard_map(
        body,
        mesh=mesh,
        in_specs=(P("scan", None, "ascan", None), P("scan", "ascan"), P("scan", "ascan")),
        out_specs=(P("scan", "ascan", None),) * 3 + (P(),),
        check_vma=False,
    )
```

```python
import functools
import math

import jax
import jax.numpy as jnp
import numpy as np
from jax import lax
from jax.experimental import pallas as pl
from jax.experimental.pallas import tpu as pltpu
from jax.sharding import PartitionSpec as P

REPEATS = 4
BINS = 2048
BANDS = 4
TILE = 128
BAND_BINS = 512
DEPTH = 1024
TILES = DEPTH // TILE
FLOOR = 0.05 * BAND_BINS
VARIANCE_SCALE = 0.1
TINY = float(np.finfo(np.float32).tiny)

MESH = pl.DeviceIdType.MESH
CHUNK = 32
SLAB = 32
RING = 8
HELD = 4


def make_table():
    sample = np.arange(BAND_BINS, dtype=np.int32)
    depth = np.arange(DEPTH, dtype=np.int32)
    product = sample[:, None] * depth[None, :] % BINS
    angle = product.astype(np.float32) * np.float32(2.0 * math.pi / BINS)
    window = np.sin(np.float32(math.pi) * (sample.astype(np.float32) + np.float32(0.5)) / np.float32(BAND_BINS)) ** 2
    parts = np.stack([window[:, None] * np.cos(angle), window[:, None] * np.sin(angle)])
    parts = parts.reshape(2, BAND_BINS, TILE // SLAB, RING, SLAB).transpose(3, 1, 0, 2, 4)
    return jnp.asarray(parts.reshape(RING, BAND_BINS, 2 * TILE), dtype=jnp.bfloat16)


def exchange_kernel(
    n_scan, n_ascan, scans, slab,
    spectra_hbm, table_hbm, top_hbm, bottom_hbm,
    maps_ref, stat_ref,
    spectra, table, top_ref, bottom_ref, profile, sums, outbox, flow, own_stat, line_stat, stat_a, stat_b,
    spectra_sem, table_sem, surface_sem, send_sem, recv_sem, send_a, recv_a, send_b, recv_b,
):
    my_scan = lax.axis_index("scan")
    me = lax.axis_index("ascan")
    per_tile = TILE // slab
    row, place = me // RING, lax.rem(me, RING)

    def group_of(step):
        pair = step // (2 * scans)
        reach = jnp.where(pair == 0, 2, jnp.where(pair == 1, 1, 3))
        near = jnp.where(lax.rem(step, 2) == 0, reach, RING - reach)
        distance = jnp.where(step < 6 * scans, near, jnp.where(step < 7 * scans, 4, 0))
        return lax.rem(place + distance, RING)

    def scan_of(step):
        return jnp.where(step < 6 * scans, lax.rem(step // 2, scans), lax.rem(step, scans))

    def table_copy(tile):
        return pltpu.make_async_copy(table_hbm.at[tile], table.at[tile], table_sem.at[tile])

    def spectra_copy(s, band):
        bins = pl.ds(band * BAND_BINS, BAND_BINS)
        return pltpu.make_async_copy(
            spectra_hbm.at[s, :, :, bins], spectra.at[s, band], spectra_sem.at[s, band]
        )

    surface_copies = (
        pltpu.make_async_copy(top_hbm, top_ref, surface_sem.at[0]),
        pltpu.make_async_copy(bottom_hbm, bottom_ref, surface_sem.at[1]),
    )
    table_copy(group_of(0)).start()
    for band in range(BANDS):
        spectra_copy(0, band).start()

    barrier = pltpu.get_barrier_semaphore()
    for along in (4, 5, 3, 6, 2, 7, 1, 0):
        for across in (2, 1, 3, 0):
            if along or across:
                to = lax.rem(row + across, per_tile) * RING + lax.rem(place + along, RING)
                pl.semaphore_signal(barrier, inc=1, device_id=(my_scan, to), device_id_type=MESH)
    for d in range(1, n_scan):
        pl.semaphore_signal(barrier, inc=1, device_id=(lax.rem(my_scan + d, n_scan), me), device_id_type=MESH)

    for c in surface_copies:
        c.start()
    for s in range(1, scans):
        for band in range(BANDS):
            spectra_copy(s, band).start()

    @pl.loop(1, RING)
    def _(d):
        table_copy(group_of(jnp.where(d < 6, d // 2 * (2 * scans) + lax.rem(d, 2), d * scans))).start()

    flow[...] = jnp.zeros_like(flow)

    def block_copy(s, source, to):
        return pltpu.make_async_remote_copy(
            src_ref=outbox.at[to, s],
            dst_ref=maps_ref.at[:, s, :, pl.ds(pl.multiple_of(source * TILE, TILE), TILE)],
            send_sem=send_sem.at[to, s],
            recv_sem=recv_sem.at[source, s],
            device_id=(my_scan, to),
            device_id_type=MESH,
        )

    def send(group, s):
        @pl.loop(0, per_tile)
        def _(d):
            to = lax.rem(row + d, per_tile) * RING + group

            @pl.when(to != me)
            def _():
                block_copy(s, me, to).start()

            @pl.when(to == me)
            def _():
                maps_ref[:, s, :, pl.ds(pl.multiple_of(me * TILE, TILE), TILE)] = outbox[me, s]

    def band_terms(band, at):
        power, amplitude = [], []
        for r in range(REPEATS):
            rows = pl.ds(r * TILE + at, CHUNK)
            c = profile[band, rows, :TILE]
            v = profile[band, rows, TILE:]
            p = c * c + v * v
            power.append(p)
            amplitude.append(p * lax.rsqrt(jnp.maximum(p, TINY)))
        similarity = None
        for r in range(REPEATS - 1):
            root = lax.rsqrt(jnp.maximum(power[r] + power[r + 1], FLOOR))
            term = (amplitude[r] * root) * (amplitude[r + 1] * root)
            similarity = term if similarity is None else similarity + term
        first = amplitude[0] + amplitude[1]
        second = amplitude[2] + amplitude[3]
        d0 = amplitude[0] - amplitude[1]
        d1 = amplitude[2] - amplitude[3]
        d2 = first - second
        return similarity, first + second, (d0 * d0 + d1 * d1) + (d2 * d2) * 0.5

    @pl.loop(0, RING * scans)
    def _(step):
        group, s = group_of(step), scan_of(step)

        @pl.when(s == 0)
        def _():
            table_copy(group).wait()

        @pl.when((step == 0) | (step == 2))
        def _():
            for band in range(BANDS):
                spectra_copy(s, band).wait()

        weights = table[group]
        for band in range(BANDS):

            profile[band] = jnp.dot(
                spectra[s, band].reshape(REPEATS * TILE, BAND_BINS),
                weights,
                preferred_element_type=jnp.float32,
            )
            for at in range(0, TILE, CHUNK):
                terms = band_terms(band, at)
                for m in range(3):
                    rows = pl.ds(at, CHUNK)
                    sums[m, rows, :] = terms[m] if band == 0 else sums[m, rows, :] + terms[m]

        @pl.when(step == 0)
        def _():
            for c in surface_copies:
                c.wait()

        top = top_ref[pl.ds(s, 1), :]
        bottom = bottom_ref[pl.ds(s, 1), :]
        masks = []
        for q in range(per_tile):
            tile = (q * RING + group) * slab // TILE
            masks.append(((top <= tile) & (tile < bottom)).astype(jnp.float32))
        for m in range(3):
            turned = sums[m].T
            for q in range(per_tile):
                part = turned[q * slab : (q + 1) * slab]
                if m == 0:
                    part = (1.0 - part * (2.0 / (BANDS * (REPEATS - 1)))) * masks[q]
                    flow[...] += jnp.sum(part.reshape(slab // 8, 8, TILE), axis=0)
                elif m == 1:
                    part = part * (masks[q] * (1.0 / (BANDS * REPEATS * math.sqrt(BAND_BINS))))
                else:
                    part = part * (masks[q] * (0.5 / (REPEATS * BANDS * VARIANCE_SCALE * BAND_BINS)))
                outbox[q * RING + group, s, m] = part

        @pl.when(step == 1)
        def _():
            pl.semaphore_wait(barrier, n_ascan + n_scan - 2)

            @pl.loop(0, 1)
            def _(early):
                send(group_of(early), scan_of(early))

        @pl.when((step >= 1) & (step < RING * scans - HELD))
        def _():
            send(group, s)

    rows = jnp.sum((bottom_ref[...] - top_ref[...]).astype(jnp.float32), axis=0, keepdims=True)
    own_stat[pl.ds(0, 1), :] = jnp.sum(flow[...], axis=0, keepdims=True)
    own_stat[pl.ds(1, 1), :] = rows * float(TILE)
    stat_a[my_scan] = own_stat[...]

    def a_copy(source, to, k):
        return pltpu.make_async_remote_copy(
            src_ref=own_stat, dst_ref=stat_a.at[source],
            send_sem=send_a.at[k], recv_sem=recv_a.at[source],
            device_id=(to, me), device_id_type=MESH,
        )

    def b_copy(source, to, k):
        return pltpu.make_async_remote_copy(
            src_ref=line_stat, dst_ref=stat_b.at[source],
            send_sem=send_b.at[k], recv_sem=recv_b.at[source],
            device_id=(my_scan, to), device_id_type=MESH,
        )

    @pl.loop(1, n_scan)
    def _(d):
        a_copy(my_scan, lax.rem(my_scan + d, n_scan), d).start()

    @pl.loop(1, n_scan)
    def _(d):
        a_copy(lax.rem(my_scan + d, n_scan), lax.rem(my_scan + d, n_scan), d).wait_recv()

    line_stat[...] = jnp.sum(stat_a[...], axis=0)
    stat_b[me] = line_stat[...]

    @pl.loop(1, n_ascan)
    def _(d):
        b_copy(me, lax.rem(me + d, n_ascan), d).start()

    @pl.loop(RING * scans - HELD, RING * scans)
    def _(step):
        send(group_of(step), scan_of(step))

    @pl.loop(1, n_scan)
    def _(d):
        a_copy(my_scan, lax.rem(my_scan + d, n_scan), d).wait_send()

    @pl.loop(1, n_ascan)
    def _(d):
        other = lax.rem(me + d, n_ascan)
        b_copy(other, other, d).wait_recv()

    totals = jnp.sum(jnp.sum(stat_b[...], axis=0), axis=1, keepdims=True)
    mean = totals[0:1] / totals[1:2]
    stat_ref[pl.ds(0, 1), :] = jnp.broadcast_to(mean, (1, TILE))
    stat_ref[pl.ds(1, 1), :] = jnp.broadcast_to(1.0 / (3.0 * mean), (1, TILE))

    @pl.loop(1, n_ascan)
    def _(d):
        other = lax.rem(me + d, n_ascan)
        b_copy(me, other, d).wait_send()
        for s in range(scans):
            block_copy(s, me, other).wait_send()

    @pl.loop(1, n_ascan)
    def _(d):
        other = lax.rem(me + d, n_ascan)
        for s in range(scans):
            block_copy(s, other, other).wait_recv()


def finish_kernel(maps_ref, stat_ref, angiogram_ref, structure_ref, speckle_ref, mean_ref, smooth, plain_sem, smooth_sem):
    scans, slab, width = angiogram_ref.shape
    block = smooth.shape[2]
    copies = [
        pltpu.make_async_copy(maps_ref.at[1], structure_ref, plain_sem.at[0]),
        pltpu.make_async_copy(maps_ref.at[2], speckle_ref, plain_sem.at[1]),
    ]
    for c in copies:
        c.start()
    mean_ref[...] = stat_ref[pl.ds(0, 1), pl.ds(0, 1)]
    scale = jnp.tile(jnp.broadcast_to(stat_ref[pl.ds(1, 1), :], (8, TILE)), (1, maps_ref.shape[3] // TILE))
    lane = lax.broadcasted_iota(jnp.int32, (8, width), 1)
    for s in range(scans):
        for k in range(slab // block):
            for z in range(0, block, 8):
                x = maps_ref[0, s, pl.ds(k * block + z, 8), :]
                before = jnp.where(lane == 0, 0.0, pltpu.roll(x, 1, 1))
                after = jnp.where(lane == width - 1, 0.0, pltpu.roll(x, width - 1, 1))
                smooth[s, k, pl.ds(z, 8), :] = (before + x + after) * scale
            c = pltpu.make_async_copy(
                smooth.at[s, k], angiogram_ref.at[s, pl.ds(k * block, block)], smooth_sem.at[s, k]
            )
            c.start()
            copies.append(c)
    for c in copies:
        c.wait()


def solution(mesh):
    n_scan, n_ascan = mesh.shape["scan"], mesh.shape["ascan"]

    def body(spectra, top, bottom):
        scans, repeats, lines, bins = spectra.shape
        slab = DEPTH // n_ascan
        width = lines * n_ascan
        f32 = jnp.float32
        vmem = pl.BlockSpec(memory_space=pltpu.VMEM)
        hbm = pl.BlockSpec(memory_space=pltpu.HBM)
        maps, stat = pl.pallas_call(
            functools.partial(exchange_kernel, n_scan, n_ascan, scans, slab),
            out_shape=(
                jax.ShapeDtypeStruct((3, scans, slab, width), f32),
                jax.ShapeDtypeStruct((2, TILE), f32),
            ),
            in_specs=[hbm] * 4,
            out_specs=(vmem, vmem),
            scratch_shapes=[
                pltpu.VMEM((scans, BANDS, REPEATS, TILE, BAND_BINS), jnp.bfloat16),
                pltpu.VMEM((RING, BAND_BINS, 2 * TILE), jnp.bfloat16),
                pltpu.VMEM((scans, TILE), jnp.int32),
                pltpu.VMEM((scans, TILE), jnp.int32),
                pltpu.VMEM((BANDS, REPEATS * TILE, 2 * TILE), f32),
                pltpu.VMEM((3, TILE, TILE), f32),
                pltpu.VMEM((n_ascan, scans, 3, slab, TILE), f32),
                pltpu.VMEM((8, TILE), f32),
                pltpu.VMEM((2, TILE), f32),
                pltpu.VMEM((2, TILE), f32),
                pltpu.VMEM((n_scan, 2, TILE), f32),
                pltpu.VMEM((n_ascan, 2, TILE), f32),
                pltpu.SemaphoreType.DMA((scans, BANDS)),
                pltpu.SemaphoreType.DMA((RING,)),
                pltpu.SemaphoreType.DMA((2,)),
                pltpu.SemaphoreType.DMA((n_ascan, scans)),
                pltpu.SemaphoreType.DMA((n_ascan, scans)),
                pltpu.SemaphoreType.DMA((n_scan,)),
                pltpu.SemaphoreType.DMA((n_scan,)),
                pltpu.SemaphoreType.DMA((n_ascan,)),
                pltpu.SemaphoreType.DMA((n_ascan,)),
            ],
            compiler_params=pltpu.CompilerParams(
                collective_id=0, has_side_effects=True, vmem_limit_bytes=40 * 2**20
            ),
            name="exchange",
        )(*(pltpu.with_memory_space_constraint(a, pltpu.HBM) for a in (spectra, make_table(), top, bottom)))

        angiogram, structure, speckle, mean = pl.pallas_call(
            finish_kernel,
            out_shape=[jax.ShapeDtypeStruct((scans, slab, width), f32)] * 3
            + [jax.ShapeDtypeStruct((1, 1), f32)],
            in_specs=[vmem, vmem],
            out_specs=[hbm] * 3 + [vmem],
            scratch_shapes=[
                pltpu.VMEM((scans, slab // 16, 16, width), f32),
                pltpu.SemaphoreType.DMA((2,)),
                pltpu.SemaphoreType.DMA((scans, slab // 16)),
            ],
            compiler_params=pltpu.CompilerParams(vmem_limit_bytes=8 * 2**20),
            name="finish",
        )(maps, stat)
        return angiogram, structure, speckle, mean.reshape(())

    return jax.shard_map(
        body,
        mesh=mesh,
        in_specs=(P("scan", None, "ascan", None), P("scan", "ascan"), P("scan", "ascan")),
        out_specs=(P("scan", "ascan", None),) * 3 + (P(),),
        check_vma=False,
    )
```
